16 devices in a mesh: dp: 2 (over z), ep: 8 (over y, x, core).
Axes of the slice: x: 2, y: 2, z: 2, core: 2. Of those that a mesh axis runs over, the one named last changes fastest.
Arguments:
- x: bfloat16 [32768, 2048], P(('dp', 'ep')), parts along dimension 0
- route_idx: int32 [32768, 8], P(('dp', 'ep')), parts along dimension 0
- gates: bfloat16 [32768, 8], P(('dp', 'ep')), parts along dimension 0
- w1: bfloat16 [72, 2048, 1024], P('ep')
- w3: bfloat16 [72, 2048, 1024], P('ep')
- w2: bfloat16 [72, 1024, 2048], P('ep')
Outputs:
- output: bfloat16 [32768, 2048], P(('dp', 'ep')), parts along dimension 0
There are 2 independent parts. The reference program is written for one: setup_inputs(seed, part) draws one part's arguments, and reference() takes and returns one part's arrays. A program takes and returns all parts, laid end to end along the dimension named above; an argument that names none is the same for every part.
All inputs are finite; a program needn't handle non-finite values.
Results may differ from the reference program's by a relative error of at most 0.0014.
Values are sent between devices in bfloat16 or wider.
A program may use at most 1 GiB of HBM per device.

```python
import jax
import jax.numpy as jnp
from jax import lax

EXPERTS = 64
TOP = 8
D = 2048
FF = 1024
TOKENS_DEV = 2048
EP = 8
BLK = 128

LOC = EXPERTS // EP
SLOTS = LOC + 1
TOKENS = EP * TOKENS_DEV
HOLDERS = [0, (EP // 2 + 1) % EP, (EP // 4 + 2) % EP, (3 * EP // 4 + 3) % EP]


def slot_table(w):
    w = w.astype(jnp.bfloat16).reshape((EP, LOC) + w.shape[1:])
    keep = jnp.zeros((EP, 1, 1), jnp.bfloat16).at[jnp.array(HOLDERS[1:])].set(1.0)
    spare = keep * w[0, 0][None]
    return jnp.concatenate([w, spare[:, None]], axis=1).reshape((EP * SLOTS,) + w.shape[2:])


def setup_inputs(seed: int = 0, part: int = 0) -> dict:
    base = jax.random.fold_in(jax.random.key(seed), part)
    ks = jax.random.split(base, 8)
    kd = jax.random.split(jax.random.fold_in(base, 7), 10)
    kw = jax.random.split(jax.random.key(seed + 1), 3)
    x = jax.random.normal(ks[0], (TOKENS, D), jnp.float32).astype(jnp.bfloat16)
    dens_bits = jax.random.bits(kd[1], (EP, 1), jnp.uint32) >> 8
    dens_cut = jnp.where(dens_bits < 5033165, jnp.uint32(1 << 24), jnp.uint32(838861) + (dens_bits * 2) // 5)
    hot = (jax.random.bits(kd[2], (EP, TOKENS_DEV), jnp.uint32) >> 8) < dens_cut
    off = jax.random.randint(kd[3], (EP, 1, 1), 0, EP)
    step = jnp.where(jax.random.uniform(kd[8], (EP, 1, 1), jnp.float32) < 0.5, 1, EP - 1)
    n = jnp.arange(TOKENS_DEV * TOP).reshape(1, TOKENS_DEV, TOP)
    dev = (off + n * step) % EP
    pop_exp = jax.random.randint(kd[4], (EP, LOC), 0, 13)
    pop_weight = jnp.left_shift(jnp.int32(1), pop_exp).at[0, 0].set(0)
    cum_weight = jnp.cumsum(pop_weight[dev], axis=-1)
    pick_draw = jax.random.randint(kd[5], dev.shape, 0, cum_weight[..., -1])
    local_pick = jnp.sum((pick_draw[..., None] >= cum_weight).astype(jnp.int32), axis=-1)
    cold = dev * LOC + local_pick
    last = jnp.arange(TOP).reshape(1, 1, TOP) == TOP - 1
    e = jnp.where(jnp.logical_and(hot[:, :, None], last), 0, cold).reshape(TOKENS, TOP)
    glogv = jax.random.normal(ks[6], (TOKENS, TOP), jnp.float32) + 0.5 * (e == 0)
    g = jax.nn.softmax(glogv, axis=-1)
    perm = (jnp.arange(TOP)[None, :] + jax.random.randint(kd[7], (TOKENS, 1), 0, TOP)) % TOP
    return dict(
        x=x,
        route_idx=jnp.take_along_axis(e, perm, axis=1).astype(jnp.int32),
        gates=jnp.take_along_axis(g, perm, axis=1).astype(jnp.bfloat16),
        w1=slot_table(jax.random.normal(kw[0], (EXPERTS, D, FF), jnp.float32) * D ** -0.5),
        w3=slot_table(jax.random.normal(kw[1], (EXPERTS, D, FF), jnp.float32) * D ** -0.5),
        w2=slot_table(jax.random.normal(kw[2], (EXPERTS, FF, D), jnp.float32) * FF ** -0.5),
    )


def grouped_ffn(xs, tok, gid, w1, w3, w2):
    n = gid.shape[0]
    d = xs.shape[1]
    g = w1.shape[0]
    nblk = -(-n // BLK) + g
    cnt = jnp.zeros((g + 1,), jnp.int32).at[gid].add(1)[:g]
    padc = (cnt + BLK - 1) // BLK * BLK
    pend = jnp.cumsum(padc)
    pstart = pend - padc
    cstart = jnp.cumsum(cnt) - cnt
    order = jnp.argsort(gid).astype(jnp.int32)
    gs = gid[order]
    gc = jnp.minimum(gs, g - 1)
    pos = jnp.where(gs < g, pstart[gc] + jnp.arange(n, dtype=jnp.int32) - cstart[gc], nblk * BLK)
    src = jnp.full((nblk * BLK,), n, jnp.int32).at[pos].set(order, mode="drop")
    bexp = jnp.minimum(jnp.searchsorted(pend, jnp.arange(nblk, dtype=jnp.int32) * BLK, side="right"), g - 1)
    used = pend[g - 1] // BLK
    xz = jnp.concatenate([xs, jnp.zeros((1, d), xs.dtype)], axis=0)
    tz = jnp.concatenate([tok, jnp.full((1,), xs.shape[0], jnp.int32)], axis=0)

    def body(b, acc):
        xb = xz[tz[lax.dynamic_slice_in_dim(src, b * BLK, BLK)]]
        ex = bexp[b]
        u = jnp.dot(xb, w1[ex], preferred_element_type=jnp.float32)
        v = jnp.dot(xb, w3[ex], preferred_element_type=jnp.float32)
        a = (jax.nn.silu(u) * v).astype(jnp.bfloat16)
        ob = jnp.dot(a, w2[ex], preferred_element_type=jnp.float32).astype(jnp.bfloat16)
        return lax.dynamic_update_slice_in_dim(acc, ob, b * BLK, axis=0)

    acc = lax.fori_loop(0, used, body, jnp.zeros((nblk * BLK, d), jnp.bfloat16))
    return jnp.zeros((n + 1, d), jnp.bfloat16).at[src].set(acc)[:n]


def reference(x, route_idx, gates, w1, w3, w2):
    e = route_idx.reshape(-1)
    slot = (e // LOC) * SLOTS + e % LOC
    tok = jnp.arange(TOKENS * TOP, dtype=jnp.int32) // TOP
    o = grouped_ffn(x, tok, slot, w1, w3, w2).reshape(TOKENS, TOP, D)
    y = jnp.zeros((TOKENS, D), jnp.float32)
    for m in range(TOP):
        y = y + gates[:, m:m + 1].astype(jnp.float32) * o[:, m].astype(jnp.float32)
    return y.astype(jnp.bfloat16)
```

```python
import functools

import jax
import jax.numpy as jnp
from jax import lax
from jax.experimental import pallas as pl
from jax.experimental.pallas import tpu as pltpu
from jax.sharding import PartitionSpec as P

CHUNKS = 4
GR = 16
GB = 16
BR = GR * GB
WT = 512
SP = 16


def holder_list(p):
    return [0, (p // 2 + 1) % p, (p // 4 + 2) % p, (3 * p // 4 + 3) % p]


def pack_kernel(wid, nblk, pos_ref, x_ref, o_ref, *, slots):
    j = pl.program_id(0)

    @pl.when(j < nblk[0])
    def _():
        pack_block(j, pos_ref, x_ref, o_ref, slots)


def pack_block(j, pos_ref, x_ref, o_ref, slots):
    rows = lax.broadcasted_iota(jnp.int32, (BR, WT), 0) + j * BR
    oh = pos_ref[0:1, :] == rows
    for s in range(1, slots):
        oh = jnp.logical_or(oh, pos_ref[s:s + 1, :] == rows)
    oh = jnp.where(oh, 1.0, 0.0).astype(jnp.bfloat16)
    d = x_ref.shape[1]
    step = 512
    for n in range(0, d, step):
        r = jnp.dot(oh, x_ref[:, n:n + step], preferred_element_type=jnp.float32)
        o_ref[:, :, n:n + step] = r.astype(jnp.bfloat16).reshape(GB, GR, step)


def pack(wid, nblk, pos, x, ng, slots):
    d = x.shape[1]
    return pl.pallas_call(
        functools.partial(pack_kernel, slots=slots),
        grid_spec=pltpu.PrefetchScalarGridSpec(
            num_scalar_prefetch=2,
            grid=wid.shape,
            in_specs=[
                pl.BlockSpec((SP, WT), lambda j, wid, nb: (0, wid[j])),
                pl.BlockSpec((WT, d), lambda j, wid, nb: (wid[j], 0)),
            ],
            out_specs=pl.BlockSpec((GB, GR, d), lambda j, wid, nb: (jnp.minimum(j, nb[0] - 1), 0, 0)),
        ),
        out_shape=jax.ShapeDtypeStruct((ng, GR, d), jnp.bfloat16),
        cost_estimate=pl.CostEstimate(flops=2 * 24 * BR * WT * d, bytes_accessed=24 * BR * d * 4, transcendentals=0),
        name="pack",
    )(wid, nblk, pos, x)


def ffn_kernel(bexp, grp, nb, xs, w1, w3, w2, o, xbuf, obuf, abuf, isem, osem):
    i = pl.program_id(0)
    n = nb[0]

    @pl.when(i < n)
    def _():
        ffn_block(i, n, grp, xs, w1, w3, w2, o, xbuf, obuf, abuf, isem, osem)


def ffn_block(i, n, grp, xs, w1, w3, w2, o, xbuf, obuf, abuf, isem, osem):
    slot = lax.rem(i, 2)

    def start_in(b, sl):
        for g in range(GB):
            pltpu.make_async_copy(xs.at[grp[b * GB + g]], xbuf.at[sl, g], isem.at[sl]).start()

    @pl.when(i == 0)
    def _():
        start_in(0, 0)

    @pl.when(i + 1 < n)
    def _():
        start_in(i + 1, 1 - slot)

    pltpu.make_async_copy(xs.at[pl.ds(0, GB)], xbuf.at[slot], isem.at[slot]).wait()

    @pl.when(i >= 2)
    def _():
        pltpu.make_async_copy(obuf.at[slot], o.at[pl.ds(0, GB)], osem.at[slot]).wait()

    d = xs.shape[2]
    ff = w1.shape[2]
    x = xbuf[slot].reshape(BR, d)
    step = 256
    for c in range(0, ff, step):
        u = jnp.dot(x, w1[0, :, c:c + step], preferred_element_type=jnp.float32)
        v = jnp.dot(x, w3[0, :, c:c + step], preferred_element_type=jnp.float32)
        abuf[:, c:c + step] = (jax.nn.silu(u) * v).astype(jnp.bfloat16)
    a = abuf[...]
    step = 512
    for c in range(0, d, step):
        r = jnp.dot(a, w2[0, :, c:c + step], preferred_element_type=jnp.float32)
        obuf[slot, :, :, c:c + step] = r.astype(jnp.bfloat16).reshape(GB, GR, step)

    for g in range(GB):
        pltpu.make_async_copy(obuf.at[slot, g], o.at[grp[i * GB + g]], osem.at[slot]).start()

    @pl.when(i == n - 1)
    def _():
        pltpu.make_async_copy(obuf.at[slot], o.at[pl.ds(0, GB)], osem.at[slot]).wait()

        @pl.when(i >= 1)
        def _():
            pltpu.make_async_copy(obuf.at[1 - slot], o.at[pl.ds(0, GB)], osem.at[1 - slot]).wait()


def ffn(bexp, grp, nb, xs, w1, w3, w2):
    ng, _, d = xs.shape
    ff = w1.shape[2]
    return pl.pallas_call(
        ffn_kernel,
        grid_spec=pltpu.PrefetchScalarGridSpec(
            num_scalar_prefetch=3,
            grid=bexp.shape,
            in_specs=[
                pl.BlockSpec(memory_space=pl.ANY),
                pl.BlockSpec((1, d, ff), lambda i, be, gr, nb: (be[i], 0, 0)),
                pl.BlockSpec((1, d, ff), lambda i, be, gr, nb: (be[i], 0, 0)),
                pl.BlockSpec((1, ff, d), lambda i, be, gr, nb: (be[i], 0, 0)),
            ],
            out_specs=pl.BlockSpec(memory_space=pl.ANY),
            scratch_shapes=[
                pltpu.VMEM((2, GB, GR, d), jnp.bfloat16),
                pltpu.VMEM((2, GB, GR, d), jnp.bfloat16),
                pltpu.VMEM((BR, ff), jnp.bfloat16),
                pltpu.SemaphoreType.DMA((2,)),
                pltpu.SemaphoreType.DMA((2,)),
            ],
        ),
        out_shape=jax.ShapeDtypeStruct((ng, GR, d), jnp.bfloat16),
        compiler_params=pltpu.CompilerParams(vmem_limit_bytes=56 * 2 ** 20),
        cost_estimate=pl.CostEstimate(flops=6 * 24 * BR * d * ff, bytes_accessed=24 * BR * d * 4, transcendentals=0),
        name="ffn",
    )(bexp, grp, nb, xs, w1, w3, w2)


def combine_kernel(wid, first, nval, nblk, pos_ref, gate_ref, o_ref, y_ref, *, slots):
    j = pl.program_id(0)

    @pl.when(j < nblk[0])
    def _():
        combine_block(j, first, nval, pos_ref, gate_ref, o_ref, y_ref, slots)


def combine_block(j, first, nval, pos_ref, gate_ref, o_ref, y_ref, slots):
    rows = lax.broadcasted_iota(jnp.int32, (BR, WT), 0) + j * BR
    gm = jnp.zeros((BR, WT), jnp.float32)
    for s in range(slots):
        gm = jnp.where(pos_ref[s:s + 1, :] == rows, gate_ref[s:s + 1, :], gm)
    gm = gm.astype(jnp.bfloat16)
    d = y_ref.shape[1]
    step = 512
    live = lax.broadcasted_iota(jnp.int32, (BR, step), 0) < nval[j]
    for c in range(0, d, step):
        o = o_ref[:, :, c:c + step].reshape(BR, step)
        o = jnp.where(live, o, jnp.zeros((), jnp.bfloat16))
        r = lax.dot_general(gm, o, (((0,), (0,)), ((), ())), preferred_element_type=jnp.float32)

        @pl.when(first[j] == 1)
        def _():
            y_ref[:, c:c + step] = r

        @pl.when(first[j] == 0)
        def _():
            y_ref[:, c:c + step] += r


def combine(wid, first, nval, nblk, pos, gate, o, slots):
    d = o.shape[2]
    t = pos.shape[1]
    return pl.pallas_call(
        functools.partial(combine_kernel, slots=slots),
        grid_spec=pltpu.PrefetchScalarGridSpec(
            num_scalar_prefetch=4,
            grid=wid.shape,
            in_specs=[
                pl.BlockSpec((SP, WT), lambda j, wid, f, v, nb: (0, wid[j])),
                pl.BlockSpec((SP, WT), lambda j, wid, f, v, nb: (0, wid[j])),
                pl.BlockSpec((GB, GR, d), lambda j, wid, f, v, nb: (jnp.minimum(j, nb[0] - 1), 0, 0)),
            ],
            out_specs=pl.BlockSpec((WT, d), lambda j, wid, f, v, nb: (wid[j], 0)),
        ),
        out_shape=jax.ShapeDtypeStruct((t, d), jnp.float32),
        cost_estimate=pl.CostEstimate(flops=2 * 24 * BR * WT * d, bytes_accessed=24 * BR * d * 8, transcendentals=0),
        name="combine",
    )(wid, first, nval, nblk, pos, gate, o)


def solution(mesh):
    p = mesh.shape["ep"]
    hold = holder_list(p)
    nh = len(hold)
    table = [hold.index(q) if q in hold else nh for q in range(p)]

    def local(x, ridx, gates, w1, w3, w2):
        td, d = x.shape
        k = ridx.shape[1]
        slots = w1.shape[0]
        loc = slots - 1
        nc = CHUNKS
        tc = td // nc
        tch = tc * p
        nw = tch // WT
        me = lax.axis_index("ep")
        gme = jnp.array(table, jnp.int32)[me]

        rmax = p * min(td * k // p, tc * k) + -(-tch // nh)
        gmax = rmax // GR + nw * slots
        wbmax = gmax // GB + nw
        ebmax = gmax // GB + slots
        ng = (wbmax + 2) * GB
        trash = wbmax * GB

        def chunked(v):
            a = lax.all_gather(v.T, "ep", axis=1, tiled=False)
            return a.reshape(k, p, nc, tc).transpose(0, 2, 1, 3).reshape(k, nc * tch)
        rt = chunked(ridx)
        gt = chunked(gates).astype(jnp.float32)
        s_id = jnp.arange(slots, dtype=jnp.int32)
        eid = jnp.where(s_id < loc, me * loc + s_id, jnp.where(jnp.logical_and(gme < nh, me != 0), 0, -1))
        share = jnp.arange(nc * tch, dtype=jnp.int32) % nh == gme
        match = rt[:, None, :] == eid[None, :, None]
        match = jnp.logical_and(match, jnp.logical_or(eid[None, :, None] != 0, share[None, None, :]))
        sel = jnp.any(match, axis=0)
        gate = jnp.sum(jnp.where(match, gt[:, None, :], 0.0), axis=0)
        selb = sel.astype(jnp.bfloat16).reshape(slots * nc * nw, WT)
        tri = (jnp.arange(WT)[:, None] < jnp.arange(WT)[None, :]).astype(jnp.bfloat16)
        rank = jnp.dot(selb, tri, preferred_element_type=jnp.float32).astype(jnp.int32)
        rank = rank.reshape(slots, nc, nw, WT)
        selw = sel.reshape(slots, nc, nw, WT)
        cnt = rank[..., -1] + selw[..., -1].astype(jnp.int32)
        n_g = ((cnt + GR - 1) // GR).transpose(1, 2, 0)
        g_off = jnp.cumsum(n_g, axis=2) - n_g
        g_w = jnp.sum(n_g, axis=2)
        nb_w = jnp.maximum((g_w + GB - 1) // GB, 1)
        b_end = jnp.cumsum(nb_w, axis=1)
        b_off = b_end - nb_w
        base = b_off[:, :, None] * GB + g_off
        pos = jnp.where(selw, base.transpose(2, 0, 1)[..., None] * GR + rank, -1).reshape(slots, nc, tch)
        pos = jnp.pad(pos, ((0, SP - slots), (0, 0), (0, 0)), constant_values=-1)
        gate = jnp.pad(gate.reshape(slots, nc, tch), ((0, SP - slots), (0, 0), (0, 0)))

        jb = jnp.arange(wbmax, dtype=jnp.int32)
        wid = jnp.minimum(jnp.sum((jb[None, :, None] >= b_end[:, None, :]).astype(jnp.int32), axis=2), nw - 1)
        ohw = wid[:, :, None] == jnp.arange(nw)
        jrel = jb[None, :] - jnp.sum(jnp.where(ohw, b_off[:, None, :], 0), axis=2)
        nval = jnp.clip(jnp.sum(jnp.where(ohw, g_w[:, None, :], 0), axis=2) * GR - jrel * BR, 0, BR)
        first = (jrel == 0).astype(jnp.int32)
        nblk = b_end[:, -1:]

        w_end = jnp.cumsum(n_g, axis=1)
        tg = w_end[:, -1, :]
        nb_s = (tg + GB - 1) // GB
        e_end = jnp.cumsum(nb_s, axis=1)
        ib = jnp.arange(ebmax, dtype=jnp.int32)
        bexp = jnp.minimum(jnp.sum((ib[None, :, None] >= e_end[:, None, :]).astype(jnp.int32), axis=2), slots - 1)
        ohs = bexp[:, :, None] == s_id
        irel = ib[None, :] - jnp.sum(jnp.where(ohs, (e_end - nb_s)[:, None, :], 0), axis=2)
        q = irel[:, :, None] * GB + jnp.arange(GB, dtype=jnp.int32)
        pick = lambda v: jnp.sum(jnp.where(ohs[:, :, None, :], v[:, None, :, :], 0), axis=3)
        we, wn, wbase = pick(w_end), pick(n_g), pick(base)
        ws = we - wn
        hit = jnp.logical_and(q[..., None] >= ws[:, :, None, :], q[..., None] < we[:, :, None, :])
        src = jnp.sum(jnp.where(hit, (wbase - ws)[:, :, None, :] + q[..., None], 0), axis=3)
        spare = trash + (ib[:, None] % 2) * GB + jnp.arange(GB, dtype=jnp.int32)[None, :]
        grp = jnp.where(jnp.any(hit, axis=3), src, spare[None]).reshape(nc, ebmax * GB)
        nb = jnp.maximum(e_end[:, -1:], 1)

        ys = []
        for c in range(nc):
            xa = lax.all_gather(x[c * tc:(c + 1) * tc], "ep", axis=0, tiled=True)
            xs = pack(wid[c], nblk[c], pos[:, c], xa, ng, slots)
            o = ffn(bexp[c], grp[c], nb[c], xs, w1, w3, w2)
            yp = combine(wid[c], first[c], nval[c], nblk[c], pos[:, c], gate[:, c], o, slots)
            ys.append(lax.psum_scatter(yp, "ep", scatter_dimension=0, tiled=True).astype(jnp.bfloat16))
        return jnp.concatenate(ys, axis=0)

    spec_t = P(("dp", "ep"), None)
    spec_w = P("ep", None, None)
    return jax.shard_map(local, mesh=mesh, in_specs=(spec_t, spec_t, spec_t, spec_w, spec_w, spec_w), out_specs=spec_t, check_vma=False)
```

```python
import functools

import jax
import jax.numpy as jnp
from jax import lax
from jax.experimental import pallas as pl
from jax.experimental.pallas import tpu as pltpu
from jax.sharding import PartitionSpec as P

CHUNKS = 4
PIECES = {0: 1, 1: 1, 2: 2}
GR = 16
GB = 16
BR = GR * GB
WT = 512
SP = 16
SMEM = pl.BlockSpec(memory_space=pltpu.SMEM)
HBM = pl.BlockSpec(memory_space=pltpu.HBM)
VMEM_LIMIT = 56 * 2 ** 20


def holder_list(p):
    return [0, (p // 2 + 1) % p, (p // 4 + 2) % p, (3 * p // 4 + 3) % p]


def pack_kernel(wid, nblk, pos, xa, xb, o, *, slots, half, m, r):
    d = xa.shape[1]

    def body(pos_ref, xa_ref, xb_ref, o_ref):
        j = pl.program_id(0)

        @pl.when(wid[j] < half)
        def _():
            pack_block(j, pos_ref, xa_ref, o_ref, slots)

        @pl.when(wid[j] >= half)
        def _():
            pack_block(j, pos_ref, xb_ref, o_ref, slots)

    pltpu.emit_pipeline(
        body,
        grid=(nblk[0],),
        in_specs=[
            pl.BlockSpec((SP, WT), lambda j: (0, wid[j])),
            pl.BlockSpec((WT, d), lambda j: (jnp.minimum(wid[j], half - 1) * m + r, 0)),
            pl.BlockSpec((WT, d), lambda j: (jnp.maximum(wid[j] - half, 0) * m + r, 0)),
        ],
        out_specs=[pl.BlockSpec((GB, GR, d), lambda j: (j, 0, 0))],
    )(pos, xa, xb, o)


def pack_block(j, pos_ref, x_ref, o_ref, slots):
    rows = lax.broadcasted_iota(jnp.int32, (BR, WT), 0) + j * BR
    oh = pos_ref[0:1, :] == rows
    for s in range(1, slots):
        oh = jnp.logical_or(oh, pos_ref[s:s + 1, :] == rows)
    oh = jnp.where(oh, 1.0, 0.0).astype(jnp.bfloat16)
    d = x_ref.shape[1]
    step = 1024

    @pl.loop(0, d // step)
    def _(n):
        col = pl.ds(pl.multiple_of(n * step, step), step)
        r = jnp.dot(oh, x_ref[:, col], preferred_element_type=jnp.float32)
        o_ref[:, :, col] = r.astype(jnp.bfloat16).reshape(GB, GR, step)


def pack(wid, nblk, pos, xa, xb, ng, slots, m, r):
    d = xa.shape[1]
    half = xa.shape[0] // (m * WT)
    return pl.pallas_call(
        functools.partial(pack_kernel, slots=slots, half=half, m=m, r=r),
        in_specs=[SMEM, SMEM, HBM, HBM, HBM],
        out_specs=HBM,
        out_shape=jax.ShapeDtypeStruct((ng, GR, d), jnp.bfloat16),
        cost_estimate=pl.CostEstimate(flops=2 * 24 * BR * WT * d, bytes_accessed=24 * BR * d * 4, transcendentals=0),
        name="pack",
    )(wid, nblk, pos, xa, xb)


def ffn_kernel(bexp, grp, nb, xs, w1, w3, w2, o, xbuf, obuf, abuf, isem, osem):
    d, ff = w1.shape[1:]

    def body(w1_ref, w3_ref, w2_ref):
        ffn_block(pl.program_id(0), nb[0], grp, xs, w1_ref, w3_ref, w2_ref, o, xbuf, obuf, abuf, isem, osem)

    pltpu.emit_pipeline(
        body,
        grid=(nb[0],),
        in_specs=[
            pl.BlockSpec((1, d, ff), lambda i: (bexp[i], 0, 0)),
            pl.BlockSpec((1, d, ff), lambda i: (bexp[i], 0, 0)),
            pl.BlockSpec((1, ff, d), lambda i: (bexp[i], 0, 0)),
        ],
    )(w1, w3, w2)


def ffn_block(i, n, grp, xs, w1, w3, w2, o, xbuf, obuf, abuf, isem, osem):
    slot = lax.rem(i, 2)

    def start_in(b, sl):
        for g in range(GB):
            pltpu.make_async_copy(xs.at[grp[b * GB + g]], xbuf.at[sl, g], isem.at[sl]).start()

    @pl.when(i == 0)
    def _():
        start_in(0, 0)

    @pl.when(i + 1 < n)
    def _():
        start_in(i + 1, 1 - slot)

    pltpu.make_async_copy(xs.at[pl.ds(0, GB)], xbuf.at[slot], isem.at[slot]).wait()

    @pl.when(i >= 2)
    def _():
        pltpu.make_async_copy(obuf.at[slot], o.at[pl.ds(0, GB)], osem.at[slot]).wait()

    d = xs.shape[2]
    ff = w1.shape[2]
    x = xbuf[slot].reshape(BR, d)
    step = 256
    for c in range(0, ff, step):
        u = jnp.dot(x, w1[0, :, c:c + step], preferred_element_type=jnp.float32)
        v = jnp.dot(x, w3[0, :, c:c + step], preferred_element_type=jnp.float32)
        abuf[:, c:c + step] = (jax.nn.silu(u) * v).astype(jnp.bfloat16)
    a = abuf[...]
    step = 512
    for c in range(0, d, step):
        r = jnp.dot(a, w2[0, :, c:c + step], preferred_element_type=jnp.float32)
        obuf[slot, :, :, c:c + step] = r.astype(jnp.bfloat16).reshape(GB, GR, step)

    for g in range(GB):
        pltpu.make_async_copy(obuf.at[slot, g], o.at[grp[i * GB + g]], osem.at[slot]).start()

    @pl.when(i == n - 1)
    def _():
        pltpu.make_async_copy(obuf.at[slot], o.at[pl.ds(0, GB)], osem.at[slot]).wait()

        @pl.when(i >= 1)
        def _():
            pltpu.make_async_copy(obuf.at[1 - slot], o.at[pl.ds(0, GB)], osem.at[1 - slot]).wait()


def ffn(bexp, grp, nb, xs, w1, w3, w2):
    ng, _, d = xs.shape
    ff = w1.shape[2]
    return pl.pallas_call(
        ffn_kernel,
        in_specs=[SMEM, SMEM, SMEM, HBM, HBM, HBM, HBM],
        out_specs=HBM,
        scratch_shapes=[
            pltpu.VMEM((2, GB, GR, d), jnp.bfloat16),
            pltpu.VMEM((2, GB, GR, d), jnp.bfloat16),
            pltpu.VMEM((BR, ff), jnp.bfloat16),
            pltpu.SemaphoreType.DMA((2,)),
            pltpu.SemaphoreType.DMA((2,)),
        ],
        out_shape=jax.ShapeDtypeStruct((ng, GR, d), jnp.bfloat16),
        compiler_params=pltpu.CompilerParams(vmem_limit_bytes=VMEM_LIMIT),
        cost_estimate=pl.CostEstimate(flops=6 * 24 * BR * d * ff, bytes_accessed=24 * BR * d * 4, transcendentals=0),
        name="ffn",
    )(bexp, grp, nb, xs, w1, w3, w2)


def combine_kernel(wid, first, nval, nblk, off, pos, gate, o, y, *, slots, w0):
    d = y.shape[1]

    def body(pos_ref, gate_ref, o_ref, y_ref):
        combine_block(pl.program_id(0), off, first, nval, pos_ref, gate_ref, o_ref, y_ref, slots)

    pltpu.emit_pipeline(
        body,
        grid=(nblk[0],),
        in_specs=[
            pl.BlockSpec((SP, WT), lambda j: (0, w0 + wid[j])),
            pl.BlockSpec((SP, WT), lambda j: (0, w0 + wid[j])),
            pl.BlockSpec((GB, GR, d), lambda j: (off[0] + j, 0, 0)),
        ],
        out_specs=[pl.BlockSpec((WT, d), lambda j: (wid[j], 0))],
    )(pos, gate, o, y)


def combine_block(j, off, first, nval, pos_ref, gate_ref, o_ref, y_ref, slots):
    rows = lax.broadcasted_iota(jnp.int32, (BR, WT), 0) + (off[0] + j) * BR
    gm = jnp.zeros((BR, WT), jnp.float32)
    for s in range(slots):
        gm = jnp.where(pos_ref[s:s + 1, :] == rows, gate_ref[s:s + 1, :], gm)
    gm = gm.astype(jnp.bfloat16)
    d = y_ref.shape[1]
    step = 512
    live = lax.broadcasted_iota(jnp.int32, (BR, step), 0) < nval[j]
    keep = first[j] == 0

    @pl.loop(0, d // step)
    def _(n):
        col = pl.ds(pl.multiple_of(n * step, step), step)
        o = o_ref[:, :, col].reshape(BR, step)
        o = jnp.where(live, o, jnp.zeros((), jnp.bfloat16))
        r = lax.dot_general(gm, o, (((0,), (0,)), ((), ())), preferred_element_type=jnp.float32)
        y_ref[:, col] = r + jnp.where(keep, y_ref[:, col], 0.0)


def combine(wid, first, nval, nblk, off, pos, gate, o, slots, w0, t):
    d = o.shape[2]
    return pl.pallas_call(
        functools.partial(combine_kernel, slots=slots, w0=w0),
        in_specs=[SMEM] * 5 + [HBM] * 3,
        out_specs=HBM,
        out_shape=jax.ShapeDtypeStruct((t, d), jnp.float32),
        cost_estimate=pl.CostEstimate(flops=2 * 24 * BR * WT * d, bytes_accessed=24 * BR * d * 8, transcendentals=0),
        name="combine",
    )(wid, first, nval, nblk, off, pos, gate, o)


def solution(mesh):
    p = mesh.shape["ep"]
    hold = holder_list(p)
    nh = len(hold)
    table = [hold.index(q) if q in hold else nh for q in range(p)]

    def local(x, ridx, gates, w1, w3, w2):
        td, d = x.shape
        k = ridx.shape[1]
        slots = w1.shape[0]
        loc = slots - 1
        nc = CHUNKS
        tc = td // nc
        tch = tc * p
        nw = tch // WT
        me = lax.axis_index("ep")
        gme = jnp.array(table, jnp.int32)[me]
        core = me % 2
        teams = [[2 * i + c for i in range(p // 2)] for c in range(2)]
        swap = [(i, i ^ 1) for i in range(p)]

        rmax = p * min(td * k // p, tc * k) + -(-tch // nh)
        gmax = rmax // GR + nw * slots
        wbmax = gmax // GB + nw
        ebmax = gmax // GB + slots
        ng = (wbmax + 2) * GB
        trash = wbmax * GB

        def chunked(v):
            a = lax.all_gather(v.T, "ep", axis=1, tiled=False)
            a = a.reshape(k, p // 2, 2, nc, tc).transpose(0, 3, 2, 1, 4)
            a = jnp.where(core == 0, a, a[:, :, ::-1])
            return a.reshape(k, nc * tch)
        rt = chunked(ridx)
        gt = chunked(gates).astype(jnp.float32)
        s_id = jnp.arange(slots, dtype=jnp.int32)
        eid = jnp.where(s_id < loc, me * loc + s_id, jnp.where(jnp.logical_and(gme < nh, me != 0), 0, -1))
        share = jnp.arange(nc * tch, dtype=jnp.int32) % nh == gme
        match = rt[:, None, :] == eid[None, :, None]
        match = jnp.logical_and(match, jnp.logical_or(eid[None, :, None] != 0, share[None, None, :]))
        sel = jnp.any(match, axis=0)
        gate = jnp.sum(jnp.where(match, gt[:, None, :], 0.0), axis=0)
        selb = sel.astype(jnp.bfloat16).reshape(slots * nc * nw, WT)
        tri = (jnp.arange(WT)[:, None] < jnp.arange(WT)[None, :]).astype(jnp.bfloat16)
        rank = jnp.dot(selb, tri, preferred_element_type=jnp.float32).astype(jnp.int32)
        rank = rank.reshape(slots, nc, nw, WT)
        selw = sel.reshape(slots, nc, nw, WT)
        cnt = rank[..., -1] + selw[..., -1].astype(jnp.int32)
        n_g = ((cnt + GR - 1) // GR).transpose(1, 2, 0)
        g_off = jnp.cumsum(n_g, axis=2) - n_g
        g_w = jnp.sum(n_g, axis=2)
        nb_w = jnp.maximum((g_w + GB - 1) // GB, 1)
        b_end = jnp.cumsum(nb_w, axis=1)
        b_off = b_end - nb_w
        base = b_off[:, :, None] * GB + g_off
        pos = jnp.where(selw, base.transpose(2, 0, 1)[..., None] * GR + rank, -1).reshape(slots, nc, tch)
        pos = jnp.pad(pos, ((0, SP - slots), (0, 0), (0, 0)), constant_values=-1)
        gate = jnp.pad(gate.reshape(slots, nc, tch), ((0, SP - slots), (0, 0), (0, 0)))

        def blocks(bend, gw, njb):
            n = bend.shape[-1]
            jb = jnp.arange(njb, dtype=jnp.int32)
            boff = bend - jnp.maximum((gw + GB - 1) // GB, 1)
            w = jnp.minimum(jnp.sum((jb[:, None] >= bend[..., None, :]).astype(jnp.int32), axis=-1), n - 1)
            oh = w[..., None] == jnp.arange(n)
            jrel = jb - jnp.sum(jnp.where(oh, boff[..., None, :], 0), axis=-1)
            nval = jnp.clip(jnp.sum(jnp.where(oh, gw[..., None, :], 0), axis=-1) * GR - jrel * BR, 0, BR)
            return w, (jrel == 0).astype(jnp.int32), nval
        wid, _, _ = blocks(b_end, g_w, wbmax)
        nblk = b_end[:, -1:]
        nwh = nw // 2
        hbmax = (p // 2 * min(td * k // p, tc * k) + tch // 2 // nh) // GR + nwh * slots
        hbmax = hbmax // GB + nwh
        h_end = jnp.cumsum(nb_w.reshape(nc, 2, nwh), axis=2)
        hwid, first, nval = blocks(h_end, g_w.reshape(nc, 2, nwh), hbmax)
        hblk = h_end[:, :, -1:]
        hoff = jnp.concatenate([jnp.zeros_like(hblk[:, :1]), hblk[:, :1]], axis=1)

        w_end = jnp.cumsum(n_g, axis=1)
        tg = w_end[:, -1, :]
        nb_s = (tg + GB - 1) // GB
        e_end = jnp.cumsum(nb_s, axis=1)
        ib = jnp.arange(ebmax, dtype=jnp.int32)
        bexp = jnp.minimum(jnp.sum((ib[None, :, None] >= e_end[:, None, :]).astype(jnp.int32), axis=2), slots - 1)
        ohs = bexp[:, :, None] == s_id
        irel = ib[None, :] - jnp.sum(jnp.where(ohs, (e_end - nb_s)[:, None, :], 0), axis=2)
        q = irel[:, :, None] * GB + jnp.arange(GB, dtype=jnp.int32)
        pick = lambda v: jnp.sum(jnp.where(ohs[:, :, None, :], v[:, None, :, :], 0), axis=3)
        we, wn, wbase = pick(w_end), pick(n_g), pick(base)
        ws = we - wn
        hit = jnp.logical_and(q[..., None] >= ws[:, :, None, :], q[..., None] < we[:, :, None, :])
        src = jnp.sum(jnp.where(hit, (wbase - ws)[:, :, None, :] + q[..., None], 0), axis=3)
        spare = trash + (ib[:, None] % 2) * GB + jnp.arange(GB, dtype=jnp.int32)[None, :]
        grp = jnp.where(jnp.any(hit, axis=3), src, spare[None]).reshape(nc, ebmax * GB)
        nb = jnp.maximum(e_end[:, -1:], 1)

        ys = []
        for c in range(nc):
            if c in PIECES:
                c0, m = c, PIECES[c]
                xa = lax.all_gather(x[c0 * tc:(c0 + m) * tc], "ep", axis=0, tiled=True, axis_index_groups=teams)
                xb = lax.ppermute(xa, "ep", swap)
            xs = pack(wid[c], nblk[c], pos[:, c], xa, xb, ng, slots, m, c - c0)
            o = ffn(bexp[c], grp[c], nb[c], xs, w1, w3, w2)

            def part(h):
                return combine(hwid[c, h], first[c, h], nval[c, h], hblk[c, h], hoff[c, h], pos[:, c], gate[:, c], o, slots, h * nwh, tch // 2)
            there = lax.ppermute(part(1), "ep", swap)
            yp = part(0) + there
            y = lax.psum_scatter(yp, "ep", scatter_dimension=0, tiled=True, axis_index_groups=teams)
            ys.append(y.astype(jnp.bfloat16))
        return jnp.concatenate(ys, axis=0)

    spec_t = P(("dp", "ep"), None)
    spec_w = P("ep", None, None)
    return jax.shard_map(local, mesh=mesh, in_specs=(spec_t, spec_t, spec_t, spec_w, spec_w, spec_w), out_specs=spec_t, check_vma=False)
```
